256 devices in a mesh: rows: 64 (over y, z, core), cols: 4 (over x).
Axes of the slice: x: 4, y: 4, z: 8, core: 2. Of those that a mesh axis runs over, the one named last changes fastest.
Arguments:
- panel: float32 [131072, 256], P(('rows', 'cols')), may hold values from -17 to 17, as said below
- trailing: float32 [131072, 2048], P('rows', 'cols'), may hold values from -6 to 6
Outputs:
- rfactor: float32 [256, 256], replicated
- projected: float32 [256, 2048], P(None, 'cols')
- updated: float32 [131072, 2048], P('rows', 'cols')
The draws below stay inside these ranges and needn't reach their ends.
Inputs may be any that keep to these rules, and one draw needn't show every extreme that they name: The panel has full column rank with a moderate condition number (under 100); each column has its own scale and a part shared by all columns.
All inputs are finite; a program needn't handle non-finite values.
Results may differ from the reference program's by a relative error of at most 0.000078.
Values sent between devices are 32-bit elements; how exact they have to be, the bound alone decides.
No kernel may reach another device: no remote copies, remote signals or barrier semaphores. Data moves between devices by JAX's collectives and lax.ppermute only.
A program may use at most 64 MiB of HBM per device.

```python
import jax
import jax.numpy as jnp
from jax import lax

PANEL = 256
TRAIL = 2048
ROWS = 131072
PIECE = 512


def draw_panel(key, part):
    keys = jax.random.split(jax.random.fold_in(key, 17), 5)
    noise = jnp.clip(jax.random.normal(keys[0], (ROWS, PANEL), jnp.float32), -6.0, 6.0)
    pieces = ROWS // PIECE
    piece_of_row = jnp.arange(ROWS) // PIECE
    scales = jnp.exp(jax.random.uniform(keys[1], (PANEL,), jnp.float32, jnp.log(0.5), jnp.log(2.0)))
    common = jnp.clip(jax.random.normal(keys[2], (ROWS,), jnp.float32), -5.0, 5.0)
    tilt = jax.random.uniform(keys[3], (PANEL,), jnp.float32, -0.7, 0.7)
    boosted = jax.random.randint(keys[4], (pieces,), 0, PANEL)
    column_ids = jnp.arange(PANEL)
    boost = 1.0 + 5.0 * (column_ids[None, :] == boosted[piece_of_row][:, None]).astype(jnp.float32)
    values = (noise * scales[None, :] + common[:, None] * tilt[None, :]) * boost
    return (values / jnp.sqrt(jnp.float32(ROWS))).astype(jnp.float32)


def levels(stream_key, shape, cuts, smallest, largest):
    level, own = 1.0, jax.random.fold_in(stream_key, 6)
    for axis_at, parts in cuts:
        draws = jnp.exp(jax.random.uniform(jax.random.fold_in(own, axis_at), (parts,), jnp.float32, smallest / len(cuts), largest / len(cuts)))
        level = level * jnp.repeat(draws, shape[axis_at] // parts).reshape([-1 if axis == axis_at else 1 for axis in range(len(shape))])
    return level


def gaussian(stream_key, dims, deviation, bound, cuts=(), held_as=jnp.bfloat16):
    entries = deviation * jax.random.normal(stream_key, dims, jnp.float32)
    if cuts:
        entries = entries * levels(stream_key, dims, cuts, -0.22, 0.18)
    return jnp.clip(entries, -bound, bound).astype(held_as)


def setup_inputs(seed: int = 0) -> dict:
    arg_keys = jax.random.split(jax.random.key(seed), 3)
    return {
        "panel": draw_panel(jax.random.fold_in(arg_keys[2], 71), 0),
        "trailing": gaussian(arg_keys[1], (ROWS, TRAIL), 1.0, 6.0, ((0, 64), (1, 4)), jnp.float32),
    }


def inner(left, right):
    return lax.dot_general(left.astype(jnp.float32), right.astype(jnp.float32), (((0,), (0,)), ((), ())), precision=lax.Precision.HIGHEST, preferred_element_type=jnp.float32)

def reference(panel, trailing):
    gram = inner(panel, panel)
    rfactor = jnp.linalg.cholesky(gram).T
    basis = jax.scipy.linalg.solve_triangular(rfactor.T, panel.T, lower=True).T
    cross = inner(panel, trailing)
    projected = jax.scipy.linalg.solve_triangular(rfactor.T, cross, lower=True)
    updated = trailing - jnp.dot(basis.astype(jnp.float32), projected.astype(jnp.float32), precision=lax.Precision.HIGHEST, preferred_element_type=jnp.float32)
    return (rfactor, projected, updated)
```

```python
import jax
import jax.numpy as jnp
from jax import lax
from jax.experimental import pallas as pl
from jax.experimental.pallas import tpu as pltpu
from jax.sharding import PartitionSpec as P

NY, NZ, NC, NX = 4, 8, 2, 4
HIGHEST = lax.Precision.HIGHEST
F32 = jnp.float32


def row_id(y, z, c):
    return (y * NZ + z) * NC + c


GROUP_Y = [[row_id(y, z, c) for y in range(NY)] for z in range(NZ) for c in range(NC)]
GROUP_Z = [[row_id(y, z, c) for z in range(NZ)] for y in range(NY) for c in range(NC)]
CORE_SWAP = [(i, i ^ 1) for i in range(NY * NZ * NC)]
X_UP = [(i, (i + 1) % NX) for i in range(NX)]
X_DOWN = [(i, (i - 1) % NX) for i in range(NX)]


def dot(a, b, dims=((1,), (0,)), precision=HIGHEST):
    return lax.dot_general(a, b, (dims, ((), ())), precision=precision, preferred_element_type=F32)


def exchange(a, axis, groups=None):
    return lax.all_to_all(a, axis, 0, 0, axis_index_groups=groups, tiled=True)


def copies(a, n):
    return jnp.broadcast_to(a[None], (n, *a.shape))


def factor_block(d):
    n = 128
    slabs = n // 8
    D = [d[8 * s : 8 * s + 8, :] for s in range(slabs)]
    sub = lax.broadcasted_iota(jnp.int32, (8, n), 0)
    lane = lax.broadcasted_iota(jnp.int32, (8, n), 1)
    E = [(lane == sub + 8 * s).astype(F32) for s in range(slabs)]
    R = []
    for g in range(slabs):
        C = [[jnp.broadcast_to(D[s][:, 8 * g + k : 8 * g + k + 1], (8, n)) for s in range(g, slabs)] for k in range(8)]
        scale = jnp.zeros((8, n), F32)
        M = []
        for j in range(8):
            piv = jnp.broadcast_to(C[j][0][j : j + 1, :], (8, n))
            inv = 1.0 / piv
            root = lax.rsqrt(piv)
            root = root * (1.5 - 0.5 * piv * root * root)
            scale = jnp.where(sub == j, root, scale)
            M.append([C[j][t] * inv if t else jnp.where(sub > j, C[j][t] * inv, 0.0) for t in range(slabs - g)])
            for k in range(j + 1, 8):
                top = jnp.broadcast_to(C[k][0][j : j + 1, :], (8, n))
                for t in range(slabs - g):
                    C[k][t] = C[k][t] - M[j][t] * top
        for j in range(8):
            dj = jnp.broadcast_to(D[g][j : j + 1, :], (8, n))
            ej = jnp.broadcast_to(E[g][j : j + 1, :], (8, n))
            for t in range(slabs - g):
                D[g + t] = D[g + t] - M[j][t] * dj
                E[g + t] = E[g + t] - M[j][t] * ej
        R.append(jnp.where(lane >= sub + 8 * g, D[g] * scale, 0.0))
        E[g] = E[g] * scale
    return jnp.concatenate(R, axis=0), jnp.concatenate(E, axis=0)


def first_half(gram, r, x00):
    rr, xx = factor_block(gram[:128, :128])
    r[:, :128] = rr
    x00[...] = xx
    r[:, 128:] = dot(xx, gram[:128, 128:])


def second_half(gram, r0, x00, r, x):
    r01 = r0[:, 128:]
    r[:128, :] = r0[...]
    r[128:, :128] = jnp.zeros((128, 128), F32)
    x[:128, :128] = x00[...]
    x[:128, 128:] = jnp.zeros((128, 128), F32)
    r01t = r01.T
    left = dot(r01t, x00[...])
    s = gram[128:, 128:] - dot(r01t, r01)
    rr, xx = factor_block(s)
    r[128:, 128:] = rr
    x[128:, 128:] = xx
    x[128:, :128] = -dot(xx, left)


def factor(gram):
    half = jax.ShapeDtypeStruct((128, 256), F32)
    block = jax.ShapeDtypeStruct((128, 128), F32)
    whole = jax.ShapeDtypeStruct((256, 256), F32)
    r0, x00 = pl.pallas_call(first_half, out_shape=(half, block), name="factor_a")(gram)
    return pl.pallas_call(second_half, out_shape=(whole, whole), name="factor_b")(gram, r0, x00)


def mine_and_other(a, core):
    top, low = a[:128], a[128:]
    return jnp.where(core == 0, top, low), jnp.where(core == 0, low, top)


def sum_over_cores(a, core):
    mine, other = mine_and_other(a, core)
    return mine + lax.ppermute(other, "rows", CORE_SWAP)


def both_halves(a, core):
    other = lax.ppermute(a, "rows", CORE_SWAP)
    return jnp.concatenate([jnp.where(core == 0, a, other), jnp.where(core == 0, other, a)], axis=0)


def to_pieces(a):
    n = a.shape[1]
    h = n // 32
    return a.reshape(32 // h, h, n // 128, 128).transpose(0, 2, 1, 3).reshape(8, h, 128)


def from_pieces(a):
    h = a.shape[1]
    n = 32 * h
    return a.reshape(32 // h, n // 128, h, 128).transpose(0, 2, 1, 3).reshape(32, n)


def scatter_sum(a, core):
    n = a.shape[1]
    a = sum_over_cores(a, core)
    a = exchange(a.reshape(4, 32, n), "rows", GROUP_Y).sum(0)
    return exchange(to_pieces(a), "rows", GROUP_Z).sum(0)


def gather_back(a, core):
    a = from_pieces(exchange(copies(a, 8), "rows", GROUP_Z))
    a = exchange(copies(a, 4), "rows", GROUP_Y)
    return both_halves(a.reshape(128, a.shape[2]), core)


def shards(panel, trailing):
    x = lax.axis_index("cols")
    core = lax.axis_index("rows") % 2
    below = lax.ppermute(panel, "cols", X_UP)
    above = lax.ppermute(panel, "cols", X_DOWN)
    far_a = lax.ppermute(below[:256], "cols", X_UP)
    far_b = lax.ppermute(above[256:], "cols", X_DOWN)

    gram = dot(panel, panel, ((0,), (0,)))
    g = scatter_sum(gram, core)
    g = exchange(copies(g, 4), "cols").sum(0)
    gram = gather_back(g, core)
    rfactor, inverse = factor(gram)

    far = jnp.concatenate([far_a, far_b], axis=0)
    pieces = (panel, below, above, far)
    places = (x, (x + 3) % 4, (x + 1) % 4, (x + 2) % 4)
    cross = 0.0
    block = jnp.zeros((2048, 256), F32)
    for piece, q in zip(pieces, places):
        rows = lax.dynamic_slice(trailing, (q * 512, 0), (512, 512))
        cross = cross + dot(piece, rows, ((0,), (0,)))
        block = lax.dynamic_update_slice(block, piece, (q * 512, 0))
    cross = gather_back(scatter_sum(cross, core), core)

    projected = dot(inverse, cross)
    weights = dot(inverse, projected, ((0,), (0,)))
    updated = trailing - dot(block, weights)
    return rfactor, projected, updated


def solution(mesh):
    placed = (P(("rows", "cols"), None), P("rows", "cols"))
    return jax.shard_map(
        shards,
        mesh=mesh,
        in_specs=placed,
        out_specs=(P(), P(None, "cols"), P("rows", "cols")),
        check_vma=False,
    )
```

```python
import jax
import jax.numpy as jnp
from jax import lax
from jax.experimental import pallas as pl
from jax.experimental.pallas import tpu as pltpu
from jax.sharding import PartitionSpec as P

NY, NZ, NC, NX = 4, 8, 2, 4
HIGHEST = lax.Precision.HIGHEST
F32 = jnp.float32


def row_id(y, z, c):
    return (y * NZ + z) * NC + c


GROUP_YZ = [[row_id(y, z, c) for y in range(NY) for z in range(NZ)] for c in range(NC)]
CORE_SWAP = [(i, i ^ 1) for i in range(NY * NZ * NC)]
X_UP = [(i, (i + 1) % NX) for i in range(NX)]
X_DOWN = [(i, (i - 1) % NX) for i in range(NX)]


def dot(a, b, dims=((1,), (0,)), precision=HIGHEST):
    return lax.dot_general(a, b, (dims, ((), ())), precision=precision, preferred_element_type=F32)


def exchange(a, axis, groups=None):
    return lax.all_to_all(a, axis, 0, 0, axis_index_groups=groups, tiled=True)


def split(a):
    hi = a.astype(jnp.bfloat16)
    return hi, (a - hi.astype(F32)).astype(jnp.bfloat16)


def product(a, b):
    (ah, al), (bh, bl) = a, b
    return dot(ah, bh, precision=None) + (dot(ah, bl, precision=None) + dot(al, bh, precision=None))


def copies(a, n):
    return jnp.broadcast_to(a[None], (n, *a.shape))


def factor_block(d):
    n = 128
    slabs = n // 8
    D = [d[8 * s : 8 * s + 8, :] for s in range(slabs)]
    sub = lax.broadcasted_iota(jnp.int32, (8, n), 0)
    lane = lax.broadcasted_iota(jnp.int32, (8, n), 1)
    E = [(lane == sub + 8 * s).astype(F32) for s in range(slabs)]
    R = []
    for g in range(slabs):
        C = [[jnp.broadcast_to(D[s][:, 8 * g + k : 8 * g + k + 1], (8, n)) for s in range(g, slabs)] for k in range(8)]
        scale = jnp.zeros((8, n), F32)
        M = []
        for j in range(8):
            piv = jnp.broadcast_to(C[j][0][j : j + 1, :], (8, n))
            inv = 1.0 / piv
            root = lax.rsqrt(piv)
            root = root * (1.5 - 0.5 * piv * root * root)
            scale = jnp.where(sub == j, root, scale)
            M.append([C[j][t] * inv if t else jnp.where(sub > j, C[j][t] * inv, 0.0) for t in range(slabs - g)])
            for k in range(j + 1, 8):
                top = jnp.broadcast_to(C[k][0][j : j + 1, :], (8, n))
                for t in range(slabs - g):
                    C[k][t] = C[k][t] - M[j][t] * top
        for j in range(8):
            dj = jnp.broadcast_to(D[g][j : j + 1, :], (8, n))
            ej = jnp.broadcast_to(E[g][j : j + 1, :], (8, n))
            for t in range(slabs - g):
                D[g + t] = D[g + t] - M[j][t] * dj
                E[g + t] = E[g + t] - M[j][t] * ej
        R.append(jnp.where(lane >= sub + 8 * g, D[g] * scale, 0.0))
        E[g] = E[g] * scale
    return jnp.concatenate(R, axis=0), jnp.concatenate(E, axis=0)


def cut(src, start, out, first):
    across = src.shape[1] // 128
    h = 4 * across
    for p in range(32):
        r, c = divmod(p, across)
        out[p, first : first + h, :] = src[pl.ds(start + r * h, h), 128 * c : 128 * c + 128]


def paste(pieces, start, dst, first):
    across = dst.shape[1] // 128
    h = 4 * across
    for p in range(32):
        r, c = divmod(p, across)
        dst[pl.ds(start + r * h, h), 128 * c : 128 * c + 128] = pieces[p, first : first + h, :]


def starts(core):
    mine = pl.multiple_of(core[0] * 128, 128)
    return mine, pl.multiple_of(128 - mine, 128)


SMALL = pltpu.CompilerParams(vmem_limit_bytes=24 * 2**20)
SCALARS = pl.BlockSpec(memory_space=pltpu.SMEM)
VMEM = pl.BlockSpec(memory_space=pltpu.VMEM)


def shaped(*shape):
    return jax.ShapeDtypeStruct(shape, F32)


def first_half(core, mine, other, gram, r, x00):
    m, o = starts(core)
    paste(mine, m, gram, 16)
    paste(other, o, gram, 16)
    rr, xx = factor_block(gram[:128, :128])
    r[:, :128] = rr
    x00[...] = xx
    r[:, 128:] = dot(xx, gram[:128, 128:])


def second_half(gram, r0, x00, r, x):
    r01 = r0[:, 128:]
    r[:128, :] = r0[...]
    r[128:, :128] = jnp.zeros((128, 128), F32)
    x[:128, :128] = x00[...]
    x[:128, 128:] = jnp.zeros((128, 128), F32)
    r01t = r01.T
    left = dot(r01t, x00[...])
    s = gram[128:, 128:] - dot(r01t, r01)
    rr, xx = factor_block(s)
    r[128:, 128:] = rr
    x[128:, 128:] = xx
    x[128:, :128] = -dot(xx, left)


def factor(core, mine, other):
    gram, r0, x00 = pl.pallas_call(
        first_half,
        out_shape=(shaped(256, 256), shaped(128, 256), shaped(128, 128)),
        in_specs=[SCALARS, VMEM, VMEM],
        compiler_params=SMALL,
        name="factor_a",
    )(core, mine, other)
    return pl.pallas_call(
        second_half,
        out_shape=(shaped(256, 256), shaped(256, 256)),
        compiler_params=SMALL,
        name="factor_b",
    )(gram, r0, x00)


def accumulate(pieces, trails):
    cross, gram = 0.0, 0.0
    for piece, trail in zip(pieces, trails):
        flipped = piece.T
        cross = cross + product(split(flipped), split(trail))
        gram = gram + dot(flipped, piece)
    return cross, gram


def cross_own(places, panel, trail, cross, gram):
    cross[...], gram[...] = accumulate([panel[...]], [trail[...]])


def cross_near(places, b1, b2, a1, a2, cross0, gram0, tb, ta, cross, gram):
    c, g = accumulate([b1[...], b2[...], a1[...], a2[...]], [tb[:256, :], tb[256:, :], ta[:256, :], ta[256:, :]])
    cross[...] = cross0[...] + c
    gram[...] = gram0[...] + g


def cross_far(places, f1, f2, cross0, gram0, tf, mine, other, cross, gram):
    c, g = accumulate([f1[...], f2[...]], [tf[:256, :], tf[256:, :]])
    cross[...] = cross0[...] + c
    gram[...] = gram0[...] + g
    m, o = starts([places[4]])
    cut(cross, m, mine, 0)
    cut(gram, m, mine, 16)
    cut(cross, o, other, 0)
    cut(gram, o, other, 16)


def trail_at(k):
    return pl.BlockSpec((512, 512), lambda i, places: (places[k], 0))


def full(shape):
    return pl.BlockSpec(shape, lambda i, places: (0,) * len(shape))


def cross_call(kernel, name, places, arrays, trailing, which, outs, scratch=()):
    return pl.pallas_call(
        kernel,
        grid_spec=pltpu.PrefetchScalarGridSpec(
            num_scalar_prefetch=1,
            grid=(1,),
            in_specs=[full(a.shape) for a in arrays] + [trail_at(k) for k in which],
            out_specs=[full(o.shape) for o in outs],
            scratch_shapes=scratch,
        ),
        out_shape=outs,
        compiler_params=SMALL,
        name=name,
    )(places, *arrays, *[trailing] * len(which))


def finish(
    places, inverse, mine, other, own, b1, b2, a1, a2, f1, f2, trailing, projected, updated, cross, stage, result, reads, writes
):
    def read(k):
        rows = pl.ds(pl.multiple_of(places[k] * 512, 512), 512)
        return pltpu.make_async_copy(trailing.at[rows, :], stage.at[k], reads.at[k])

    def write(k):
        rows = pl.ds(pl.multiple_of(places[k] * 512, 512), 512)
        return pltpu.make_async_copy(result.at[k], updated.at[rows, :], writes.at[k])

    for k in range(4):
        read(k).start()
    m, o = starts([places[4]])
    paste(mine, m, cross, 0)
    paste(other, o, cross, 0)
    p = dot(inverse[...], cross[...])
    projected[...] = p
    w = split(dot(inverse[...], p, ((0,), (0,))))
    for k, parts in enumerate([(own,), (b1, b2), (a1, a2), (f1, f2)]):
        read(k).wait()
        n = 512 // len(parts)
        for i, part in enumerate(parts):
            rows = slice(n * i, n * i + n)
            result[k, rows, :] = stage[k, rows, :] - product(split(part[...]), w)
        write(k).start()
    for k in range(4):
        write(k).wait()


def finished(places, inverse, mine, other, pieces, trailing):
    return pl.pallas_call(
        finish,
        in_specs=[SCALARS] + [VMEM] * 10 + [pl.BlockSpec(memory_space=pltpu.HBM)],
        out_specs=[VMEM, pl.BlockSpec(memory_space=pltpu.HBM)],
        scratch_shapes=[pltpu.VMEM((256, 512), F32)]
        + [pltpu.VMEM((4, 512, 512), F32)] * 2
        + [pltpu.SemaphoreType.DMA((4,))] * 2,
        out_shape=(shaped(256, 512), shaped(2048, 512)),
        compiler_params=SMALL,
        name="finish",
    )(places, inverse, mine, other, *pieces, trailing)


def swap(a):
    return lax.ppermute(a, "rows", CORE_SWAP)


def shift(a, way):
    return lax.ppermute(a, "cols", way)


def shards(panel, trailing):
    x = lax.axis_index("cols")
    core = lax.axis_index("rows") % 2
    core_word = core.reshape(1)
    places = jnp.stack([x, (x + 3) % 4, (x + 1) % 4, (x + 2) % 4, core])

    top, low = panel[:256], panel[256:]
    b1 = shift(top, X_UP)
    a2 = shift(low, X_DOWN)
    b2 = shift(low, X_UP)
    a1 = shift(top, X_DOWN)

    f1 = shift(b1, X_UP)
    f2 = shift(a2, X_DOWN)
    sums = [shaped(256, 512), shaped(256, 256)]
    part = cross_call(cross_own, "cross_own", places, [panel], trailing, [0], sums)
    part = cross_call(cross_near, "cross_near", places, [b1, b2, a1, a2, *part], trailing, [1, 2], sums)
    halves = [shaped(32, 24, 128)] * 2
    scratch = [pltpu.VMEM((256, 512), F32), pltpu.VMEM((256, 256), F32)]
    mine, other = cross_call(cross_far, "cross_far", places, [f1, f2, *part], trailing, [3], halves, scratch)
    total = exchange(mine + swap(other), "rows", GROUP_YZ).sum(0)
    mine = exchange(copies(total, 32), "rows", GROUP_YZ)
    other = swap(mine)
    rfactor, inverse = factor(core_word, mine, other)
    projected, updated = finished(places, inverse, mine, other, (panel, b1, b2, a1, a2, f1, f2), trailing)
    return rfactor, projected, updated


def solution(mesh):
    placed = (P(("rows", "cols"), None), P("rows", "cols"))
    return jax.shard_map(
        shards,
        mesh=mesh,
        in_specs=placed,
        out_specs=(P(), P(None, "cols"), P("rows", "cols")),
        check_vma=False,
    )
```

```python
import jax
import jax.numpy as jnp
from jax import lax
from jax.experimental import pallas as pl
from jax.experimental.pallas import tpu as pltpu
from jax.sharding import PartitionSpec as P

NY, NZ, NC, NX = 4, 8, 2, 4
HIGHEST = lax.Precision.HIGHEST
F32 = jnp.float32


def row_id(y, z, c):
    return (y * NZ + z) * NC + c


GROUP_YZ = [[row_id(y, z, c) for y in range(NY) for z in range(NZ)] for c in range(NC)]
CORE_SWAP = [(i, i ^ 1) for i in range(NY * NZ * NC)]
X_UP = [(i, (i + 1) % NX) for i in range(NX)]
X_DOWN = [(i, (i - 1) % NX) for i in range(NX)]


def dot(a, b, dims=((1,), (0,)), precision=HIGHEST):
    return lax.dot_general(a, b, (dims, ((), ())), precision=precision, preferred_element_type=F32)


def exchange(a, axis, groups=None):
    return lax.all_to_all(a, axis, 0, 0, axis_index_groups=groups, tiled=True)


def split(a):
    hi = a.astype(jnp.bfloat16)
    return hi, (a - hi.astype(F32)).astype(jnp.bfloat16)


def product(a, b):
    (ah, al), (bh, bl) = a, b
    return dot(ah, bh, precision=None) + (dot(ah, bl, precision=None) + dot(al, bh, precision=None))


def copies(a, n):
    return jnp.broadcast_to(a[None], (n, *a.shape))


def spread(slab, row):
    return jnp.broadcast_to(slab[row : row + 1, :], slab.shape)


def factor_block(d):
    n = 128
    slabs = n // 8
    D = [d[8 * s : 8 * s + 8, :] for s in range(slabs)]
    sub = lax.broadcasted_iota(jnp.int32, (8, n), 0)
    lane = lax.broadcasted_iota(jnp.int32, (8, n), 1)
    E = [(lane == sub + 8 * s).astype(F32) for s in range(slabs)]
    R = []
    for g in range(slabs):
        C = [[jnp.broadcast_to(D[s][:, 8 * g + k : 8 * g + k + 1], (8, n)) for s in range(g, slabs)] for k in range(8)]
        scale = jnp.zeros((8, n), F32)
        M = []
        piv = spread(C[0][0], 0)
        for j in range(8):
            inv = 1.0 / piv
            if j < 7:
                after = spread(C[j + 1][0], j + 1) - (spread(C[j][0], j + 1) * inv) * spread(C[j + 1][0], j)
            root = lax.rsqrt(piv)
            root = root * (1.5 - 0.5 * piv * root * root)
            scale = jnp.where(sub == j, root, scale)
            M.append([C[j][t] * inv if t else jnp.where(sub > j, C[j][t] * inv, 0.0) for t in range(slabs - g)])
            for k in range(j + 1, 8):
                top = spread(C[k][0], j)
                for t in range(slabs - g):
                    C[k][t] = C[k][t] - M[j][t] * top
            piv = after
        for j in range(8):
            dj = spread(D[g], j)
            ej = spread(E[g], j)
            for t in range(slabs - g):
                D[g + t] = D[g + t] - M[j][t] * dj
                E[g + t] = E[g + t] - M[j][t] * ej
        R.append(jnp.where(lane >= sub + 8 * g, D[g] * scale, 0.0))
        E[g] = E[g] * scale
    return jnp.concatenate(R, axis=0), jnp.concatenate(E, axis=0)


def cut(src, start, out, first):
    across = src.shape[1] // 128
    h = 4 * across
    for p in range(32):
        r, c = divmod(p, across)
        out[p, first : first + h, :] = src[pl.ds(start + r * h, h), 128 * c : 128 * c + 128]


def paste(pieces, start, dst, first):
    across = dst.shape[1] // 128
    h = 4 * across
    for p in range(32):
        r, c = divmod(p, across)
        dst[pl.ds(start + r * h, h), 128 * c : 128 * c + 128] = pieces[p, first : first + h, :]


def starts(core):
    mine = pl.multiple_of(core[0] * 128, 128)
    return mine, pl.multiple_of(128 - mine, 128)


SMALL = pltpu.CompilerParams(vmem_limit_bytes=24 * 2**20)
FLOPS = 4 * 10**9
SCALARS = pl.BlockSpec(memory_space=pltpu.SMEM)
VMEM = pl.BlockSpec(memory_space=pltpu.VMEM)


def shaped(*shape):
    return jax.ShapeDtypeStruct(shape, F32)


def factor_kernel(core, mine, other, r, x, gram):
    m, o = starts([core[0]])
    paste(mine, m, gram, 16)
    paste(other, o, gram, 16)
    r00, x00 = factor_block(gram[:128, :128])
    r01 = dot(x00, gram[:128, 128:])
    r01t = r01.T
    r11, x11 = factor_block(gram[128:, 128:] - dot(r01t, r01))
    zero = jnp.zeros((128, 128), F32)
    r[:128, :128] = r00
    r[:128, 128:] = r01
    r[128:, :128] = zero
    r[128:, 128:] = r11
    x[:128, :128] = x00
    x[:128, 128:] = zero
    x[128:, :128] = -dot(x11, dot(r01t, x00))
    x[128:, 128:] = x11


def factor(core, mine, other):
    return pl.pallas_call(
        factor_kernel,
        out_shape=(shaped(256, 256), shaped(256, 256)),
        in_specs=[SCALARS, VMEM, VMEM],
        scratch_shapes=[pltpu.VMEM((256, 256), F32)],
        compiler_params=SMALL,
        cost_estimate=pl.CostEstimate(flops=FLOPS, bytes_accessed=2**20, transcendentals=0),
        name="factor",
    )(core, mine, other)


def accumulate(pieces, trails):
    cross, gram = 0.0, 0.0
    for piece, trail in zip(pieces, trails):
        flipped, straight = split(piece.T), split(piece)
        cross = cross + product(flipped, split(trail))
        gram = gram + (product(flipped, straight) + dot(flipped[1], straight[1], precision=None))
    return cross, gram


def rows_at(ref, place, first=0, n=512):
    return ref[pl.ds(pl.multiple_of(place * 512 + first, 256), n), :]


def cross_own(places, panel, trailing, keep, cross, gram):
    keep[...] = trailing[...]
    cross[...], gram[...] = accumulate([panel[...]], [rows_at(trailing, places[0])])


def cross_near(places, b1, b2, a1, a2, keep, cross0, gram0, cross, gram):
    trails = [rows_at(keep, places[k], first, 256) for k in (1, 2) for first in (0, 256)]
    c, g = accumulate([b1[...], b2[...], a1[...], a2[...]], trails)
    cross[...] = cross0[...] + c
    gram[...] = gram0[...] + g


def cross_far(places, f1, f2, keep, cross0, gram0, mine, other, cross, gram):
    trails = [rows_at(keep, places[3], first, 256) for first in (0, 256)]
    c, g = accumulate([f1[...], f2[...]], trails)
    cross[...] = cross0[...] + c
    gram[...] = gram0[...] + g
    m, o = starts([places[4]])
    cut(cross, m, mine, 0)
    cut(gram, m, mine, 16)
    cut(cross, o, other, 0)
    cut(gram, o, other, 16)


def call(kernel, places, arrays, outs, flops, scratch=()):
    return pl.pallas_call(
        kernel,
        in_specs=[SCALARS] + [VMEM] * len(arrays),
        out_specs=[VMEM] * len(outs),
        out_shape=outs,
        scratch_shapes=scratch,
        compiler_params=SMALL,
        cost_estimate=pl.CostEstimate(flops=flops, bytes_accessed=2**21, transcendentals=0),
        name=kernel.__name__,
    )(places, *arrays)


def finish(places, inverse, mine, other, own, b1, b2, a1, a2, f1, f2, trailing, projected, updated, cross, result, writes):
    m, o = starts([places[4]])
    paste(mine, m, cross, 0)
    paste(other, o, cross, 0)
    p = dot(inverse[...], cross[...])
    projected[...] = p
    w = split(dot(inverse[...], p, ((0,), (0,))))
    moves = []
    for k, parts in enumerate([(own,), (b1, b2), (a1, a2), (f1, f2)]):
        n = 512 // len(parts)
        for i, part in enumerate(parts):
            result[k, n * i : n * i + n, :] = rows_at(trailing, places[k], n * i, n) - product(split(part[...]), w)
        rows = pl.ds(pl.multiple_of(places[k] * 512, 512), 512)
        moves.append(pltpu.make_async_copy(result.at[k], updated.at[rows, :], writes.at[k]))
        moves[k].start()
    for move in moves:
        move.wait()


def finished(places, arrays):
    return pl.pallas_call(
        finish,
        in_specs=[SCALARS] + [VMEM] * len(arrays),
        out_specs=[VMEM, pl.BlockSpec(memory_space=pltpu.HBM)],
        out_shape=[shaped(256, 512), shaped(2048, 512)],
        scratch_shapes=[pltpu.VMEM((256, 512), F32), pltpu.VMEM((4, 512, 512), F32), pltpu.SemaphoreType.DMA((4,))],
        compiler_params=SMALL,
        name="finish",
    )(places, *arrays)


def swap(a):
    return lax.ppermute(a, "rows", CORE_SWAP)


def shift(a, way):
    return lax.ppermute(a, "cols", way)


def shards(panel, trailing):
    x = lax.axis_index("cols")
    core = lax.axis_index("rows") % 2
    core_word = core.reshape(1)
    places = jnp.stack([x, (x + 3) % 4, (x + 1) % 4, (x + 2) % 4, core])

    top, low = panel[:256], panel[256:]
    b1 = shift(top, X_UP)
    a2 = shift(low, X_DOWN)
    b2 = shift(low, X_UP)
    a1 = shift(top, X_DOWN)
    sums = [shaped(256, 512), shaped(256, 256)]
    keep, *part = call(cross_own, places, [panel, trailing], [shaped(2048, 512), *sums], 10**9)
    b1, a2, keep, *part = lax.optimization_barrier((b1, a2, keep, *part))
    f1 = shift(b1, X_UP)
    f2 = shift(a2, X_DOWN)
    part = call(cross_near, places, [b1, b2, a1, a2, keep, *part], sums, 10**8)
    halves = [shaped(32, 24, 128)] * 2
    scratch = [pltpu.VMEM((256, 512), F32), pltpu.VMEM((256, 256), F32)]
    mine, other = call(cross_far, places, [f1, f2, keep, *part], halves, 10**8, scratch)
    total = exchange(mine + swap(other), "rows", GROUP_YZ).sum(0)
    mine = exchange(copies(total, 32), "rows", GROUP_YZ)
    other = swap(mine)
    rfactor, inverse = factor(core_word, mine, other)
    projected, updated = finished(places, [inverse, mine, other, panel, b1, b2, a1, a2, f1, f2, trailing])
    return rfactor, projected, updated


def solution(mesh):
    placed = (P(("rows", "cols"), None), P("rows", "cols"))
    return jax.shard_map(
        shards,
        mesh=mesh,
        in_specs=placed,
        out_specs=(P(), P(None, "cols"), P("rows", "cols")),
        check_vma=False,
    )
```

```python
import jax
import jax.numpy as jnp
from jax import lax
from jax.experimental import pallas as pl
from jax.experimental.pallas import tpu as pltpu
from jax.sharding import PartitionSpec as P


NY, NZ, NC, NX = 4, 8, 2, 4
HIGHEST = lax.Precision.HIGHEST
F32 = jnp.float32


def row_id(y, z, c):
    return (y * NZ + z) * NC + c


GROUP_YZ = [[row_id(y, z, c) for y in range(NY) for z in range(NZ)] for c in range(NC)]
CORE_SWAP = [(i, i ^ 1) for i in range(NY * NZ * NC)]
X_UP = [(i, (i + 1) % NX) for i in range(NX)]
X_DOWN = [(i, (i - 1) % NX) for i in range(NX)]


def dot(a, b, dims=((1,), (0,)), precision=HIGHEST):
    return lax.dot_general(a, b, (dims, ((), ())), precision=precision, preferred_element_type=F32)


def exchange(a, axis, groups=None):
    return lax.all_to_all(a, axis, 0, 0, axis_index_groups=groups, tiled=True)


def split(a):
    hi = a.astype(jnp.bfloat16)
    return hi, (a - hi.astype(F32)).astype(jnp.bfloat16)


def product(a, b):
    (ah, al), (bh, bl) = a, b
    return dot(ah, bh, precision=None) + (dot(ah, bl, precision=None) + dot(al, bh, precision=None))


def copies(a, n):
    return jnp.broadcast_to(a[None], (n, *a.shape))


def spread(slab, row):
    return jnp.broadcast_to(slab[row : row + 1, :], slab.shape)


def factor_block(d):
    n = 128
    slabs = n // 8
    D = [d[8 * s : 8 * s + 8, :] for s in range(slabs)]
    sub = lax.broadcasted_iota(jnp.int32, (8, n), 0)
    lane = lax.broadcasted_iota(jnp.int32, (8, n), 1)
    E = [(lane == sub + 8 * s).astype(F32) for s in range(slabs)]
    R = []
    for g in range(slabs):
        C = [[jnp.broadcast_to(D[s][:, 8 * g + k : 8 * g + k + 1], (8, n)) for s in range(g, slabs)] for k in range(8)]
        scale = jnp.zeros((8, n), F32)
        M = []
        piv = spread(C[0][0], 0)
        for j in range(8):
            inv = 1.0 / piv
            if j < 7:
                after = spread(C[j + 1][0], j + 1) - (spread(C[j][0], j + 1) * inv) * spread(C[j + 1][0], j)
            root = lax.rsqrt(piv)
            root = root * (1.5 - 0.5 * piv * root * root)
            scale = jnp.where(sub == j, root, scale)
            M.append([C[j][t] * inv if t else jnp.where(sub > j, C[j][t] * inv, 0.0) for t in range(slabs - g)])
            for k in range(j + 1, 8):
                top = spread(C[k][0], j)
                for t in range(slabs - g):
                    C[k][t] = C[k][t] - M[j][t] * top
            piv = after
        for j in range(8):
            dj = spread(D[g], j)
            ej = spread(E[g], j)
            for t in range(slabs - g):
                D[g + t] = D[g + t] - M[j][t] * dj
                E[g + t] = E[g + t] - M[j][t] * ej
        R.append(jnp.where(lane >= sub + 8 * g, D[g] * scale, 0.0))
        E[g] = E[g] * scale
    return jnp.concatenate(R, axis=0), jnp.concatenate(E, axis=0)


def cut(src, start, out, first):
    across = src.shape[1] // 128
    h = 4 * across
    for p in range(32):
        r, c = divmod(p, across)
        out[p, first : first + h, :] = src[pl.ds(start + r * h, h), 128 * c : 128 * c + 128]


def paste(pieces, start, dst, first):
    across = dst.shape[1] // 128
    h = 4 * across
    for p in range(32):
        r, c = divmod(p, across)
        dst[pl.ds(start + r * h, h), 128 * c : 128 * c + 128] = pieces[p, first : first + h, :]


def starts(core):
    mine = pl.multiple_of(core[0] * 128, 128)
    return mine, pl.multiple_of(128 - mine, 128)


SMALL = pltpu.CompilerParams(vmem_limit_bytes=24 * 2**20)
FLOPS = 4 * 10**9
SCALARS = pl.BlockSpec(memory_space=pltpu.SMEM)
VMEM = pl.BlockSpec(memory_space=pltpu.VMEM)


def shaped(*shape):
    return jax.ShapeDtypeStruct(shape, F32)


def gram_kernel(core, panel, mine, other, whole):
    a = panel[...]
    whole[...] = dot(a.T, a)
    m, o = starts([core[0]])
    cut(whole, m, mine, 0)
    cut(whole, o, other, 0)


def gram_of(core, panel):
    return pl.pallas_call(
        gram_kernel,
        out_shape=(shaped(32, 8, 128), shaped(32, 8, 128)),
        in_specs=[SCALARS, VMEM],
        scratch_shapes=[pltpu.VMEM((256, 256), F32)],
        compiler_params=SMALL,
        name="gram",
    )(core, panel)


def factor_kernel(core, mine, other, r, x, gram):
    m, o = starts([core[0]])
    paste(mine, m, gram, 16)
    paste(other, o, gram, 0)
    r00, x00 = factor_block(gram[:128, :128])
    r01 = dot(x00, gram[:128, 128:])
    r01t = r01.T
    r11, x11 = factor_block(gram[128:, 128:] - dot(r01t, r01))
    zero = jnp.zeros((128, 128), F32)
    r[:128, :128] = r00
    r[:128, 128:] = r01
    r[128:, :128] = zero
    r[128:, 128:] = r11
    x[:128, :128] = x00
    x[:128, 128:] = zero
    x[128:, :128] = -dot(x11, dot(r01t, x00))
    x[128:, 128:] = x11


def factor(core, mine, other):
    return pl.pallas_call(
        factor_kernel,
        out_shape=(shaped(256, 256), shaped(256, 256)),
        in_specs=[SCALARS, VMEM, VMEM],
        scratch_shapes=[pltpu.VMEM((256, 256), F32)],
        compiler_params=SMALL,
        cost_estimate=pl.CostEstimate(flops=FLOPS, bytes_accessed=2**20, transcendentals=0),
        name="factor",
    )(core, mine, other)


def accumulate(pieces, trails):
    total = 0.0
    for piece, trail in zip(pieces, trails):
        total = total + product(split(piece.T), split(trail))
    return total


def rows_at(ref, place, first=0, n=512):
    return ref[pl.ds(pl.multiple_of(place * 512 + first, 256), n), :]


def cross_near(places, own, b1, b2, a1, a2, trailing, hi, lo, cross):
    trails = [rows_at(trailing, places[k], first, 256) for k in (1, 2) for first in (0, 256)]
    trails.insert(0, rows_at(trailing, places[0]))
    cross[...] = accumulate([own[...], b1[...], b2[...], a1[...], a2[...]], trails)
    hi[...], lo[...] = split(rows_at(trailing, places[3]))


def cross_far(places, f1, f2, hi, lo, cross0, mine, other, cross):
    total = cross0[...]
    for i, part in enumerate((f1, f2)):
        rows = slice(256 * i, 256 * i + 256)
        total = total + product(split(part[...].T), (hi[rows, :], lo[rows, :]))
    cross[...] = total
    m, o = starts([places[4]])
    cut(cross, m, mine, 0)
    cut(cross, o, other, 0)


def call(kernel, places, arrays, outs, flops, scratch=()):
    return pl.pallas_call(
        kernel,
        in_specs=[SCALARS] + [VMEM] * len(arrays),
        out_specs=[VMEM] * len(outs),
        out_shape=outs,
        scratch_shapes=scratch,
        compiler_params=SMALL,
        cost_estimate=pl.CostEstimate(flops=flops, bytes_accessed=2**21, transcendentals=0),
    )(places, *arrays)


def weights(places, inverse, mine, other, projected, hi, lo, cross):
    m, o = starts([places[4]])
    paste(mine, m, cross, 0)
    paste(other, o, cross, 0)
    x = inverse[...]
    p = product(split(x), split(cross[...]))
    projected[...] = p
    hi[...], lo[...] = split(product(split(x.T), split(p)))


def update(places, hi, lo, own, b1, b2, a1, a2, f1, f2, trailing, updated, result, writes):
    w = hi[...], lo[...]
    moves = []
    for k, parts in enumerate([(own,), (b1, b2), (a1, a2), (f1, f2)]):
        n = 512 // len(parts)
        for i, part in enumerate(parts):
            result[k, n * i : n * i + n, :] = rows_at(trailing, places[k], n * i, n) - product(split(part[...]), w)
        rows = pl.ds(pl.multiple_of(places[k] * 512, 512), 512)
        moves.append(pltpu.make_async_copy(result.at[k], updated.at[rows, :], writes.at[k]))
        moves[k].start()
    for move in moves:
        move.wait()


def updated_of(places, arrays):
    return pl.pallas_call(
        update,
        in_specs=[SCALARS] + [VMEM] * len(arrays),
        out_specs=pl.BlockSpec(memory_space=pltpu.HBM),
        out_shape=shaped(2048, 512),
        scratch_shapes=[pltpu.VMEM((4, 512, 512), F32), pltpu.SemaphoreType.DMA((4,))],
        compiler_params=SMALL,
        name="update",
    )(places, *arrays)


def swap(a):
    return lax.ppermute(a, "rows", CORE_SWAP)


def shift(a, way):
    return lax.ppermute(a, "cols", way)


def shards(panel, trailing):
    x = lax.axis_index("cols")
    core = lax.axis_index("rows") % 2
    core_word = core.reshape(1)
    places = jnp.stack([x, (x + 3) % 4, (x + 1) % 4, (x + 2) % 4, core])

    top, low = panel[:256], panel[256:]
    b1 = shift(top, X_UP)
    a2 = shift(low, X_DOWN)
    b2 = shift(low, X_UP)
    a1 = shift(top, X_DOWN)
    mine, other = gram_of(core_word, panel)
    g = mine + swap(other)
    g = exchange(g, "rows", GROUP_YZ)
    g = g.sum(0)
    f1 = shift(b1, X_UP)
    f2 = shift(a2, X_DOWN)
    g = exchange(copies(g, 4), "cols")
    half = jax.ShapeDtypeStruct((512, 512), jnp.bfloat16)
    part = call(cross_near, places, [panel, b1, b2, a1, a2, trailing], [half, half, shaped(256, 512)], 10**9)
    g = g.sum(0)
    halves = [shaped(32, 16, 128)] * 2
    scratch = [pltpu.VMEM((256, 512), F32)]
    mine, other = call(cross_far, places, [f1, f2, *part], halves, 10**8, scratch)
    both = exchange(jnp.concatenate([mine + swap(other), copies(g, 32)], axis=1), "rows", GROUP_YZ)
    mine = exchange(copies(both[:, :16].sum(0), 32), "rows", GROUP_YZ)
    rfactor, inverse = factor(core_word, both, swap(both[:, 16:]))
    inverse, mine = lax.optimization_barrier((inverse, mine))
    other = swap(mine)
    small = jax.ShapeDtypeStruct((256, 512), jnp.bfloat16)
    outs = [shaped(256, 512), small, small]
    projected, hi, lo = call(weights, places, [inverse, mine, other], outs, FLOPS, [pltpu.VMEM((256, 512), F32)])
    updated = updated_of(places, [hi, lo, panel, b1, b2, a1, a2, f1, f2, trailing])
    return rfactor, projected, updated


def solution(mesh):
    placed = (P(("rows", "cols"), None), P("rows", "cols"))

    return jax.shard_map(
        shards,
        mesh=mesh,
        in_specs=placed,
        out_specs=(P(), P(None, "cols"), P("rows", "cols")),
        check_vma=False,
    )
```

```python
import jax
import jax.numpy as jnp
from jax import lax
from jax.experimental import pallas as pl
from jax.experimental.pallas import tpu as pltpu
from jax.sharding import PartitionSpec as P


NY, NZ, NC, NX = 4, 8, 2, 4
HIGHEST = lax.Precision.HIGHEST
F32 = jnp.float32


def row_id(y, z, c):
    return (y * NZ + z) * NC + c


GROUP_YZ = [[row_id(y, z, c) for y in range(NY) for z in range(NZ)] for c in range(NC)]
CORE_SWAP = [(i, i ^ 1) for i in range(NY * NZ * NC)]
X_UP = [(i, (i + 1) % NX) for i in range(NX)]
X_ACROSS = [(i, (i + 2) % NX) for i in range(NX)]
X_DOWN = [(i, (i - 1) % NX) for i in range(NX)]


def dot(a, b, dims=((1,), (0,)), precision=HIGHEST):
    return lax.dot_general(a, b, (dims, ((), ())), precision=precision, preferred_element_type=F32)


def exchange(a, axis, groups=None):
    return lax.all_to_all(a, axis, 0, 0, axis_index_groups=groups, tiled=True)


def split(a):
    hi = a.astype(jnp.bfloat16)
    return hi, (a - hi.astype(F32)).astype(jnp.bfloat16)


def product(a, b):
    (ah, al), (bh, bl) = a, b
    return dot(ah, bh, precision=None) + (dot(ah, bl, precision=None) + dot(al, bh, precision=None))


def copies(a, n):
    return jnp.broadcast_to(a[None], (n, *a.shape))


def spread(slab, row):
    return jnp.broadcast_to(slab[row : row + 1, :], slab.shape)


def factor_block(d):
    n = 128
    slabs = n // 8
    D = [d[8 * s : 8 * s + 8, :] for s in range(slabs)]
    sub = lax.broadcasted_iota(jnp.int32, (8, n), 0)
    lane = lax.broadcasted_iota(jnp.int32, (8, n), 1)
    E = [(lane == sub + 8 * s).astype(F32) for s in range(slabs)]
    R = []
    for g in range(slabs):
        C = [[jnp.broadcast_to(D[s][:, 8 * g + k : 8 * g + k + 1], (8, n)) for s in range(g, slabs)] for k in range(8)]
        scale = jnp.zeros((8, n), F32)
        M = []
        piv = spread(C[0][0], 0)
        for j in range(8):
            inv = 1.0 / piv
            if j < 7:
                after = spread(C[j + 1][0], j + 1) - (spread(C[j][0], j + 1) * inv) * spread(C[j + 1][0], j)
            root = lax.rsqrt(piv)
            root = root * (1.5 - 0.5 * piv * root * root)
            scale = jnp.where(sub == j, root, scale)
            M.append([C[j][t] * inv if t else jnp.where(sub > j, C[j][t] * inv, 0.0) for t in range(slabs - g)])
            for k in range(j + 1, 8):
                top = spread(C[k][0], j)
                for t in range(slabs - g):
                    C[k][t] = C[k][t] - M[j][t] * top
            piv = after
        for j in range(8):
            dj = spread(D[g], j)
            ej = spread(E[g], j)
            for t in range(slabs - g):
                D[g + t] = D[g + t] - M[j][t] * dj
                E[g + t] = E[g + t] - M[j][t] * ej
        R.append(jnp.where(lane >= sub + 8 * g, D[g] * scale, 0.0))
        E[g] = E[g] * scale
    return jnp.concatenate(R, axis=0), jnp.concatenate(E, axis=0)


def cut(src, start, out, first):
    across = src.shape[1] // 128
    h = 4 * across
    for p in range(32):
        r, c = divmod(p, across)
        out[p, first : first + h, :] = src[pl.ds(start + r * h, h), 128 * c : 128 * c + 128]


def paste(pieces, start, dst, first):
    across = dst.shape[1] // 128
    h = 4 * across
    for p in range(32):
        r, c = divmod(p, across)
        dst[pl.ds(start + r * h, h), 128 * c : 128 * c + 128] = pieces[p, first : first + h, :]


def starts(core):
    mine = pl.multiple_of(core[0] * 128, 128)
    return mine, pl.multiple_of(128 - mine, 128)


SMALL = pltpu.CompilerParams(vmem_limit_bytes=24 * 2**20)
FLOPS = 4 * 10**9
SCALARS = pl.BlockSpec(memory_space=pltpu.SMEM)
VMEM = pl.BlockSpec(memory_space=pltpu.VMEM)


def shaped(*shape):
    return jax.ShapeDtypeStruct(shape, F32)


def gram_kernel(core, panel, mine, other, whole):
    a = panel[...]
    whole[...] = dot(a.T, a)
    m, o = starts([core[0]])
    cut(whole, m, mine, 0)
    cut(whole, o, other, 0)


def gram_of(core, panel):
    return pl.pallas_call(
        gram_kernel,
        out_shape=(shaped(32, 8, 128), shaped(32, 8, 128)),
        in_specs=[SCALARS, VMEM],
        scratch_shapes=[pltpu.VMEM((256, 256), F32)],
        compiler_params=SMALL,
        name="gram",
    )(core, panel)


def factor_kernel(core, mine, other, r, x, gram):
    m, o = starts([core[0]])
    paste(mine, m, gram, 16)
    paste(other, o, gram, 0)
    r00, x00 = factor_block(gram[:128, :128])
    r01 = dot(x00, gram[:128, 128:])
    r01t = r01.T
    r11, x11 = factor_block(gram[128:, 128:] - dot(r01t, r01))
    zero = jnp.zeros((128, 128), F32)
    r[:128, :128] = r00
    r[:128, 128:] = r01
    r[128:, :128] = zero
    r[128:, 128:] = r11
    x[:128, :128] = x00
    x[:128, 128:] = zero
    x[128:, :128] = -dot(x11, dot(r01t, x00))
    x[128:, 128:] = x11


def factor(core, mine, other):
    return pl.pallas_call(
        factor_kernel,
        out_shape=(shaped(256, 256), shaped(256, 256)),
        in_specs=[SCALARS, VMEM, VMEM],
        scratch_shapes=[pltpu.VMEM((256, 256), F32)],
        compiler_params=SMALL,
        cost_estimate=pl.CostEstimate(flops=FLOPS, bytes_accessed=2**20, transcendentals=0),
        name="factor",
    )(core, mine, other)


def accumulate(pieces, trails):
    total = 0.0
    for piece, trail in zip(pieces, trails):
        total = total + product(split(piece.T), split(trail))
    return total


def rows_at(ref, place, first=0, n=512):
    return ref[pl.ds(pl.multiple_of(place * 512 + first, 256), n), :]


def cross_near(places, own, b1, b2, a1, a2, trailing, hi, lo, cross):
    trails = [rows_at(trailing, places[k], first, 256) for k in (1, 2) for first in (0, 256)]
    trails.insert(0, rows_at(trailing, places[0]))
    cross[...] = accumulate([own[...], b1[...], b2[...], a1[...], a2[...]], trails)
    hi[...], lo[...] = split(rows_at(trailing, places[3]))


def cross_far(places, f1, f2, hi, lo, cross0, mine, other, cross):
    total = cross0[...]
    for i, part in enumerate((f1, f2)):
        rows = slice(256 * i, 256 * i + 256)
        total = total + product(split(part[...].T), (hi[rows, :], lo[rows, :]))
    cross[...] = total
    m, o = starts([places[4]])
    cut(cross, m, mine, 0)
    cut(cross, o, other, 0)


def call(kernel, places, arrays, outs, flops, scratch=()):
    return pl.pallas_call(
        kernel,
        in_specs=[SCALARS] + [VMEM] * len(arrays),
        out_specs=[VMEM] * len(outs),
        out_shape=outs,
        scratch_shapes=scratch,
        compiler_params=SMALL,
        cost_estimate=pl.CostEstimate(flops=flops, bytes_accessed=2**21, transcendentals=0),
    )(places, *arrays)


def weights(places, inverse, mine, other, projected, hi, lo, cross):
    m, o = starts([places[4]])
    paste(mine, m, cross, 0)
    paste(other, o, cross, 0)
    x = inverse[...]
    p = product(split(x), split(cross[...]))
    projected[...] = p
    hi[...], lo[...] = split(product(split(x.T), split(p)))


def update(places, hi, lo, own, b1, b2, a1, a2, f1, f2, trailing, updated, result, writes):
    w = hi[...], lo[...]
    moves = []
    for k, parts in enumerate([(own,), (b1, b2), (a1, a2), (f1, f2)]):
        n = 512 // len(parts)
        for i, part in enumerate(parts):
            result[k, n * i : n * i + n, :] = rows_at(trailing, places[k], n * i, n) - product(split(part[...]), w)
        rows = pl.ds(pl.multiple_of(places[k] * 512, 512), 512)
        moves.append(pltpu.make_async_copy(result.at[k], updated.at[rows, :], writes.at[k]))
        moves[k].start()
    for move in moves:
        move.wait()


def updated_of(places, arrays):
    return pl.pallas_call(
        update,
        in_specs=[SCALARS] + [VMEM] * len(arrays),
        out_specs=pl.BlockSpec(memory_space=pltpu.HBM),
        out_shape=shaped(2048, 512),
        scratch_shapes=[pltpu.VMEM((4, 512, 512), F32), pltpu.SemaphoreType.DMA((4,))],
        compiler_params=SMALL,
        name="update",
    )(places, *arrays)


def swap(a):
    return lax.ppermute(a, "rows", CORE_SWAP)


def shift(a, way):
    return lax.ppermute(a, "cols", way)


def shards(panel, trailing):
    x = lax.axis_index("cols")
    core = lax.axis_index("rows") % 2
    core_word = core.reshape(1)
    places = jnp.stack([x, (x + 3) % 4, (x + 1) % 4, (x + 2) % 4, core])

    top, low = panel[:256], panel[256:]
    b1 = shift(top, X_UP)
    a2 = shift(low, X_DOWN)
    b2 = shift(low, X_UP)
    a1 = shift(top, X_DOWN)
    mine, other = gram_of(core_word, panel)
    g = mine + swap(other)
    g = exchange(g, "rows", GROUP_YZ)
    g = g.sum(0)
    f1 = shift(b1, X_UP)
    f2 = shift(a2, X_DOWN)
    g1, g2, g3 = shift(g, X_UP), shift(g, X_DOWN), shift(g, X_ACROSS)
    half = jax.ShapeDtypeStruct((512, 512), jnp.bfloat16)
    part = call(cross_near, places, [panel, b1, b2, a1, a2, trailing], [half, half, shaped(256, 512)], 10**9)
    g = (g + g3) + (g1 + g2)
    halves = [shaped(32, 16, 128)] * 2
    scratch = [pltpu.VMEM((256, 512), F32)]
    mine, other = call(cross_far, places, [f1, f2, *part], halves, 10**8, scratch)
    both = exchange(jnp.concatenate([mine + swap(other), copies(g, 32)], axis=1), "rows", GROUP_YZ)
    mine = exchange(copies(both[:, :16].sum(0), 32), "rows", GROUP_YZ)
    rfactor, inverse = factor(core_word, both, swap(both[:, 16:]))
    inverse, mine = lax.optimization_barrier((inverse, mine))
    other = swap(mine)
    small = jax.ShapeDtypeStruct((256, 512), jnp.bfloat16)
    outs = [shaped(256, 512), small, small]
    projected, hi, lo = call(weights, places, [inverse, mine, other], outs, FLOPS, [pltpu.VMEM((256, 512), F32)])
    updated = updated_of(places, [hi, lo, panel, b1, b2, a1, a2, f1, f2, trailing])
    return rfactor, projected, updated


def solution(mesh):
    placed = (P(("rows", "cols"), None), P("rows", "cols"))

    return jax.shard_map(
        shards,
        mesh=mesh,
        in_specs=placed,
        out_specs=(P(), P(None, "cols"), P("rows", "cols")),
        check_vma=False,
    )
```
